32 devices in a mesh: ctx: 8 (over z, y), dp: 4 (over x, core).
Axes of the slice: x: 2, y: 2, z: 4, core: 2. Of those that a mesh axis runs over, the one named last changes fastest.
Arguments:
- grad_out: bfloat16 [4, 3072, 4096], P('dp', 'ctx'), may hold values from -6 to 6
- hidden: bfloat16 [4, 3072, 1792], P('dp', 'ctx'), may hold values from -6 to 6
- down_weight: bfloat16 [1792, 4096], replicated, may hold values from -0.09375 to 0.09375
Outputs:
- grad_hidden: bfloat16 [4, 3072, 1792], P('dp', 'ctx')
- weight_grad: float32 [1792, 4096], P('ctx', 'dp')
- hidden_amax: float32 [4, 1792], P('dp', 'ctx')
- grad_amax: float32 [4, 4096], P('dp', 'ctx')
The draws below stay inside these ranges and needn't reach their ends.
All inputs are finite; a program needn't handle non-finite values.
Results may differ from the reference program's by a relative error of at most 0.006.
Values may be sent and summed in bfloat16 or wider, within the bound.
No kernel may reach another device: no remote copies, remote signals or barrier semaphores. Data moves between devices by JAX's collectives and lax.ppermute only.
A program may use at most 192 MiB of HBM per device.

```python
import jax
import jax.numpy as jnp
from jax import lax

D = 4096
FFS = 1792
SEQ = 3072
REPLICAS = 4


def level_of(own_key, dims, pieces, low, top_value):
    level, own = 1.0, jax.random.fold_in(own_key, 6)
    for dim, shards_of in pieces:
        heights = jnp.exp(jax.random.uniform(jax.random.fold_in(own, dim), (shards_of,), jnp.float32, low / len(pieces), top_value / len(pieces)))
        level = level * jnp.repeat(heights, dims[dim] // shards_of).reshape([-1 if axis == dim else 1 for axis in range(len(dims))])
    return level


def noise(stream_key, extent, spread, reach, split=(), dtype=jnp.bfloat16):
    array = spread * jax.random.normal(stream_key, extent, jnp.float32)
    if split:
        array = array * level_of(stream_key, extent, split, -0.22, 0.18)
    return jnp.clip(array, -reach, reach).astype(dtype)


def setup_inputs(seed: int = 0) -> dict:
    key_list = jax.random.split(jax.random.key(seed), 4)
    grad_out = noise(key_list[0], (REPLICAS, SEQ, D), 1.0, 6.0, ((0, 4), (1, 8)))
    hidden = noise(key_list[1], (REPLICAS, SEQ, FFS), 1.0, 6.0, ((0, 4), (1, 8)))
    down_weight = noise(key_list[2], (FFS, D), D ** -0.5, 0.09375)
    return dict(grad_out=grad_out, hidden=hidden, down_weight=down_weight)


ceiling = 448.0

def to_grid(values, peaks):
    scaled = values.astype(jnp.float32) * (ceiling / peaks)[None, :]
    magnitude = jnp.abs(scaled)
    spacing = jnp.full_like(magnitude, 2.0 ** (-9))
    for exponent in range(-5, 9):
        spacing = jnp.where(magnitude >= 2.0 ** exponent, 2.0 ** (exponent - 3), spacing)
    snapped = jnp.floor(magnitude / spacing + 0.5) * spacing
    return jnp.where(scaled < 0, -snapped, snapped).astype(jnp.bfloat16)

def reference(grad_out, hidden, down_weight):
    hidden_amax = jnp.maximum(lax.optimization_barrier(jnp.max(jnp.abs(hidden.astype(jnp.float32)), axis=1)), 1.0)
    grad_amax = jnp.maximum(lax.optimization_barrier(jnp.max(jnp.abs(grad_out.astype(jnp.float32)), axis=1)), 1.0)
    total = jnp.zeros((FFS, D), jnp.float32)
    results = []
    for replica in range(REPLICAS):
        gdata = grad_out[replica]
        hdata = hidden[replica]
        results.append(lax.dot_general(gdata, down_weight, (((1,), (1,)), ((), ())), preferred_element_type=jnp.float32).astype(jnp.bfloat16))
        hquant = to_grid(hdata, hidden_amax[replica])
        gquant = to_grid(gdata, grad_amax[replica])
        product = lax.dot_general(hquant, gquant, (((0,), (0,)), ((), ())), preferred_element_type=jnp.float32)
        total = total + product * (hidden_amax[replica] / ceiling)[:, None] * (grad_amax[replica] / ceiling)[None, :]
    weight_grad = total / jnp.sqrt(jnp.float32(SEQ * REPLICAS))
    grad_hidden = jnp.stack(results, axis=0)
    return (grad_hidden, weight_grad, hidden_amax, grad_amax)
```

```python
import jax
import jax.numpy as jnp
from jax import lax
from jax.experimental import pallas as pl
from jax.experimental.pallas import tpu as pltpu
from jax.sharding import PartitionSpec as P


ceiling = 448.0
LANES = 128


def to_grid(values, factor, scale):
    scaled = values.astype(jnp.float32) * factor
    magnitude = jnp.abs(scaled)
    wide = magnitude * (2.0**23 + 1.0)
    base = jnp.maximum(wide - wide * (1.0 - 2.0**-24), 2.0**-6)
    magic = base * (1.5 * 2.0**20)
    near = (scaled + magic) - magic
    short = magnitude - jnp.abs(near)
    tie = short >= base * (0.0625 * (1.0 - 2.0**-24))
    near = jnp.where(tie, scaled + (scaled - near), near)
    return (near * scale).astype(jnp.bfloat16)


def row_order(count):
    order, bit = [0], count
    while bit > 1:
        bit //= 2
        order = [k ^ bit for k in order] + order
    return order


def turn_rows(hdata, blocks, ctx_count):
    tokens, ff = hdata.shape
    rows = ff // ctx_count
    wide = ff // 2 if (ff // 2) % LANES == 0 else LANES
    steps = ff // wide

    def body(order, source, sent, kept, peaks, turned):
        step = pl.program_id(0)
        tile = source[...]
        peaks[...] = jnp.max(jnp.abs(tile.astype(jnp.float32)), axis=0, keepdims=True)
        turned[pl.ds(pl.multiple_of(step * wide, wide), wide), :] = tile.T

        @pl.when(step == steps - 1)
        def _():
            for half, target in enumerate((sent, kept)):
                for j in range(ctx_count // 2):
                    block = order[half * (ctx_count // 2) + j]
                    start = pl.multiple_of(block * rows, 16)
                    target[j * rows : (j + 1) * rows, :] = turned[pl.ds(start, rows), :]

    half_shape = jax.ShapeDtypeStruct((ff // 2, tokens), jnp.bfloat16)
    return pl.pallas_call(
        body,
        out_shape=(half_shape, half_shape, jax.ShapeDtypeStruct((1, ff), jnp.float32)),
        grid_spec=pltpu.PrefetchScalarGridSpec(
            num_scalar_prefetch=1,
            grid=(steps,),
            in_specs=[pl.BlockSpec((tokens, wide), lambda i, o: (0, i))],
            out_specs=[
                pl.BlockSpec((ff // 2, tokens), lambda i, o: (0, 0)),
                pl.BlockSpec((ff // 2, tokens), lambda i, o: (0, 0)),
                pl.BlockSpec((1, wide), lambda i, o: (0, i)),
            ],
            scratch_shapes=[pltpu.VMEM((ff, tokens), jnp.bfloat16)],
        ),
        name="turn_rows",
    )(blocks, hdata)


def divide(peak):
    quotient = ceiling / peak
    wide = quotient * 4097.0
    high = wide - (wide - quotient)
    rest = (ceiling - high * peak) - (quotient - high) * peak
    return quotient + rest * (quotient * (1.0 / ceiling))


def scale_tables(peaks, where_to, ff, own_cols, ctx_count):
    count = len(peaks)
    rows = ff // ctx_count

    def body(where_ref, *refs):
        sources, (cols, gtable), (by_lane, by_row) = refs[:count], refs[count : count + 2], refs[count + 2 :]
        start = pl.multiple_of(ff + where_ref[ctx_count] * own_cols, LANES)
        for r in range(count):
            peak = sources[r][:, :ff]
            by_lane[r : r + 1, :] = divide(peak)
            by_lane[count + r : count + r + 1, :] = peak / ceiling
            peak = sources[r][:, pl.ds(start, own_cols)]
            gtable[r : r + 1, :] = divide(peak)
            gtable[count + r : count + r + 1, :] = peak / ceiling
        for c in range(0, ff, LANES):
            by_row[c : c + LANES, :] = by_lane[:, c : c + LANES].T
        for j in range(ctx_count):
            begin = pl.multiple_of(where_ref[j] * rows, 8)
            cols[j * rows : (j + 1) * rows, :] = by_row[pl.ds(begin, rows), :]

    whole = lambda i, w: (0, 0)
    return pl.pallas_call(
        body,
        out_shape=(
            jax.ShapeDtypeStruct((ff, 2 * count), jnp.float32),
            jax.ShapeDtypeStruct((2 * count, own_cols), jnp.float32),
        ),
        grid_spec=pltpu.PrefetchScalarGridSpec(
            num_scalar_prefetch=1,
            grid=(1,),
            in_specs=[pl.BlockSpec(peaks[0].shape, whole)] * count,
            out_specs=[pl.BlockSpec((ff, 2 * count), whole), pl.BlockSpec((2 * count, own_cols), whole)],
            scratch_shapes=[pltpu.VMEM((2 * count, ff), jnp.float32), pltpu.VMEM((ff, 2 * count), jnp.float32)],
        ),
        name="scale_tables",
    )(where_to, *peaks)


def quantize_rows(sources, cols, offset, tile):
    rows, tokens = sources[0].shape
    count = len(sources)

    def body(*refs):
        cols_ref, out = refs[count], refs[count + 1]
        for r in range(count):
            out[:, r * tokens : (r + 1) * tokens] = to_grid(
                refs[r][...], cols_ref[:, r : r + 1], cols_ref[:, count + r : count + r + 1]
            )

    return pl.pallas_call(
        body,
        out_shape=jax.ShapeDtypeStruct((rows, count * tokens), jnp.bfloat16),
        grid=(rows // tile,),
        in_specs=[pl.BlockSpec((tile, tokens), lambda i: (i, 0))] * count
        + [pl.BlockSpec((tile, 2 * count), lambda i: (i + offset // tile, 0))],
        out_specs=pl.BlockSpec((tile, count * tokens), lambda i: (i, 0)),
        cost_estimate=pl.CostEstimate(
            flops=2000 * rows * tokens * count, transcendentals=0, bytes_accessed=4 * rows * tokens * count
        ),
        name="quantize_rows",
    )(*sources, cols)


def product(left, right):
    return lax.dot_general(left, right, (((1,), (0,)), ((), ())), preferred_element_type=jnp.float32)


def quantize_and_multiply(hq, sources, gtable, start, tile):
    rows, depth = hq.shape
    tokens, width = sources[2].shape
    count = len(sources)

    def body(*refs):
        hq_ref, table = refs[:2]
        raw = refs[2 : 2 + count]
        out, gq = refs[2 + count :]

        @pl.when(pl.program_id(0) == 0)
        def _():
            for r in range(count):
                gq[r * tokens : (r + 1) * tokens, :] = to_grid(
                    raw[r][:, start : start + width] if r < 2 else raw[r][...],
                    table[r : r + 1, start : start + width],
                    table[count + r : count + r + 1, start : start + width],
                )

        out[...] = product(hq_ref[...], gq[...]).astype(jnp.bfloat16)

    whole = lambda i: (0, 0)
    return pl.pallas_call(
        body,
        out_shape=(
            jax.ShapeDtypeStruct((rows, width), jnp.bfloat16),
            jax.ShapeDtypeStruct((depth, width), jnp.bfloat16),
        ),
        grid=(rows // tile,),
        in_specs=[pl.BlockSpec((tile, depth), lambda i: (i, 0)), pl.BlockSpec(gtable.shape, whole)]
        + [pl.BlockSpec(source.shape, whole) for source in sources],
        out_specs=[pl.BlockSpec((tile, width), lambda i: (i, 0)), pl.BlockSpec((depth, width), whole)],
        cost_estimate=pl.CostEstimate(
            flops=4 * rows * depth * width, transcendentals=0, bytes_accessed=2 * depth * (rows + width)
        ),
        name="quantize_and_multiply",
    )(hq, gtable, *sources)


def finish(rows_in, cols, gq, arrived, tile):
    raw = isinstance(rows_in, list)
    inputs = rows_in if raw else [rows_in]
    count = len(inputs)
    rows, tokens = inputs[0].shape
    depth, width = gq.shape
    steps = rows // tile
    cut = steps // 2

    def body(*refs):
        gq_ref, arrived_ref = refs[:2]
        sources, rest = refs[2 : 2 + count], refs[2 + count :]
        step = pl.program_id(0)
        if raw:
            cols_ref, send, keep, hq = rest
            for r in range(count):
                hq[:, r * tokens : (r + 1) * tokens] = to_grid(
                    sources[r][...], cols_ref[:, r : r + 1], cols_ref[:, count + r : count + r + 1]
                )
        else:
            send, keep = rest
            hq = sources[0]
        total = product(hq[...], gq_ref[...]) + arrived_ref[...].astype(jnp.float32)

        @pl.when(step < cut)
        def _():
            send[...] = total.astype(jnp.bfloat16)

        @pl.when(step >= cut)
        def _():
            keep[...] = total

    by_step = lambda i: (i, 0)
    in_specs = [pl.BlockSpec((depth, width), lambda i: (0, 0)), pl.BlockSpec((tile, width), by_step)]
    in_specs += [pl.BlockSpec((tile, tokens), by_step)] * count
    operands = [gq, arrived] + inputs
    out_shape = [
        jax.ShapeDtypeStruct((cut * tile, width), jnp.bfloat16),
        jax.ShapeDtypeStruct((cut * tile, width), jnp.float32),
    ]
    out_specs = [
        pl.BlockSpec((tile, width), lambda i: (jnp.minimum(i, cut - 1), 0)),
        pl.BlockSpec((tile, width), lambda i: (jnp.maximum(i - cut, 0), 0)),
    ]
    if raw:
        in_specs.append(pl.BlockSpec((tile, 2 * count), lambda i: (i + steps, 0)))
        operands.append(cols)
        out_shape.append(jax.ShapeDtypeStruct((rows, depth), jnp.bfloat16))
        out_specs.append(pl.BlockSpec((tile, depth), by_step))
    return pl.pallas_call(
        body,
        out_shape=out_shape,
        grid=(steps,),
        in_specs=in_specs,
        out_specs=out_specs,
        cost_estimate=pl.CostEstimate(
            flops=4 * rows * depth * width, transcendentals=0, bytes_accessed=2 * depth * (rows + width)
        ),
        name="finish",
    )(*operands)


def split_width(width, parts):
    units = width // LANES
    parts = min(parts, units)
    sizes = [units // parts + (1 if i < units % parts else 0) for i in range(parts)]
    return [size * LANES for size in sizes]


def on_device(grad_out, hidden, down_weight):
    gdata = grad_out[0]
    hdata = hidden[0]
    tokens = gdata.shape[0]
    ctx_count, dp_count = lax.axis_size("ctx"), lax.axis_size("dp")
    position, place = lax.axis_index("ctx"), lax.axis_index("dp")
    ff, width = hdata.shape[1], gdata.shape[1]
    ff_rows, width_cols = ff // ctx_count, width // ctx_count
    own_cols = width // dp_count
    seq_total = tokens * ctx_count * dp_count
    tile = 2 * ff_rows

    def swap(value, axis, distance):
        count = ctx_count if axis == "ctx" else dp_count
        return lax.ppermute(value, axis, [(i, i ^ distance) for i in range(count)])

    sizes = split_width(own_cols, 3)
    starts = [sum(sizes[:j]) for j in range(len(sizes))]

    def column_block(k, start, size):
        return lax.dynamic_slice(gdata, (0, (place ^ k) * own_cols + start), (tokens, size))

    own_block = column_block(0, 0, own_cols)
    near_block = swap(column_block(1, 0, own_cols), "dp", 1)
    chunks = []
    for start, size in zip(starts, sizes):
        parts = [own_block, near_block]
        for k in range(2, dp_count):
            parts.append(swap(column_block(k, start, size), "dp", k))
        chunks.append(parts)

    blocks = position ^ jnp.array(row_order(ctx_count), jnp.int32)
    sent_rows, kept_rows, hpeak = turn_rows(hdata, blocks, ctx_count)

    def spread(value):
        slots = [value, swap(value, "dp", 1)]
        for k in range(2, dp_count, 2):
            far = swap(value, "dp", k)
            slots += [far, swap(far, "dp", 1)]
        return slots

    sent_slots = spread(sent_rows)
    kept_slots = spread(kept_rows)

    gpeak = jnp.max(jnp.abs(gdata.astype(jnp.float32)), axis=0, keepdims=True)
    peaks = jnp.concatenate([hpeak, gpeak], axis=1)
    bit = 1
    while bit < ctx_count:
        peaks = jnp.maximum(peaks, swap(peaks, "ctx", bit))
        bit *= 2
    peaks = jnp.maximum(peaks, 1.0)
    hidden_amax = lax.dynamic_slice(peaks, (0, position * ff_rows), (1, ff_rows))
    grad_amax = lax.dynamic_slice(peaks, (0, ff + position * width_cols), (1, width_cols))
    all_peaks = [peaks] + [swap(peaks, "dp", k) for k in range(1, dp_count)]
    where_to = jnp.concatenate([blocks, place[None]])
    cols, gtable = scale_tables(all_peaks, where_to, ff, own_cols, ctx_count)
    hq_sent = quantize_rows(sent_slots, cols, 0, ff_rows)
    rows_in, results = kept_slots, []
    for j, (start, size) in enumerate(zip(starts, sizes)):
        outgoing, gq = quantize_and_multiply(hq_sent, chunks[j], gtable, start, tile)
        arrived = swap(outgoing, "ctx", 1)
        send, keep, *quantized = finish(rows_in, cols, gq, arrived, ff_rows)
        rows_in = quantized[0] if quantized else rows_in
        bit = 2
        while True:
            arrived = swap(send, "ctx", bit)
            total = keep + arrived.astype(jnp.float32)
            bit *= 2
            if bit == ctx_count:
                break
            cut = total.shape[0] // 2
            send, keep = total[:cut].astype(jnp.bfloat16), total[cut:]
        results.append(total)
    weight_grad = jnp.concatenate(results, axis=1) / jnp.sqrt(jnp.float32(seq_total))

    result = lax.dot_general(
        gdata, down_weight, (((1,), (1,)), ((), ())), preferred_element_type=jnp.float32
    )
    grad_hidden = result.astype(jnp.bfloat16)[None]
    return (grad_hidden, weight_grad, hidden_amax, grad_amax)


def solution(mesh):
    placed = (P("dp", "ctx", None), P("dp", "ctx", None), P())

    return jax.shard_map(
        on_device,
        mesh=mesh,
        in_specs=placed,
        out_specs=(P("dp", "ctx", None), P("ctx", "dp"), P("dp", "ctx"), P("dp", "ctx")),
        check_vma=False,
    )
```

```python
import jax
import jax.numpy as jnp
from jax import lax
from jax.experimental import pallas as pl
from jax.experimental.pallas import tpu as pltpu
from jax.sharding import PartitionSpec as P


ceiling = 448.0
LANES = 128
PARAMS = pltpu.CompilerParams(vmem_limit_bytes=24 * 2**20)


def to_grid(values, factor, scale):
    scaled = values.astype(jnp.float32) * factor
    magnitude = jnp.abs(scaled)
    wide = magnitude * (2.0**23 + 1.0)
    base = jnp.maximum(wide - wide * (1.0 - 2.0**-24), 2.0**-6)
    magic = base * (1.5 * 2.0**20)
    near = (scaled + magic) - magic
    short = magnitude - jnp.abs(near)
    tie = short >= base * (0.0625 * (1.0 - 2.0**-24))
    near = jnp.where(tie, scaled + (scaled - near), near)
    return (near * scale).astype(jnp.bfloat16)


def row_order(count):
    order, bit = [0], count
    while bit > 1:
        bit //= 2
        order = [k ^ bit for k in order] + order
    return order


def turn_rows(hdata, where_to, ctx_count):
    tokens, ff = hdata.shape
    rows = ff // ctx_count
    wide = ff // 2 if (ff // 2) % LANES == 0 else LANES
    steps = ff // wide

    def body(where_ref, source, sent, kept, peaks, turned):
        step = pl.program_id(0)
        tile = source[...]
        peaks[...] = jnp.max(jnp.abs(tile.astype(jnp.float32)), axis=0, keepdims=True)
        turned[pl.ds(pl.multiple_of(step * wide, wide), wide), :] = tile.T

        @pl.when(step == steps - 1)
        def _():
            for half, target in enumerate((sent, kept)):
                for j in range(ctx_count // 2):
                    block = where_ref[0] ^ row_order(ctx_count)[half * (ctx_count // 2) + j]
                    start = pl.multiple_of(block * rows, 16)
                    target[j * rows : (j + 1) * rows, :] = turned[pl.ds(start, rows), :]

    half_shape = jax.ShapeDtypeStruct((ff // 2, tokens), jnp.bfloat16)
    return pl.pallas_call(
        body,
        out_shape=(half_shape, half_shape, jax.ShapeDtypeStruct((1, ff), jnp.float32)),
        grid_spec=pltpu.PrefetchScalarGridSpec(
            num_scalar_prefetch=1,
            grid=(steps,),
            in_specs=[pl.BlockSpec((tokens, wide), lambda i, o: (0, i))],
            out_specs=[
                pl.BlockSpec((ff // 2, tokens), lambda i, o: (0, 0)),
                pl.BlockSpec((ff // 2, tokens), lambda i, o: (0, 0)),
                pl.BlockSpec((1, wide), lambda i, o: (0, i)),
            ],
            scratch_shapes=[pltpu.VMEM((ff, tokens), jnp.bfloat16)],
        ),
        compiler_params=PARAMS,
        name="turn_rows",
    )(where_to, hdata)


def split_columns(gdata, where_to, dp_count, sizes):
    tokens, width = gdata.shape
    own_cols = width // dp_count
    shapes = [(tokens, own_cols)] * 2 + [(tokens, size) for _ in range(2, dp_count) for size in sizes]

    def body(where_ref, source, *refs):
        peaks, outs = refs[-1], refs[:-1]
        tile = source[...]
        peaks[...] = jnp.max(jnp.abs(tile.astype(jnp.float32)), axis=0, keepdims=True)
        for k in range(dp_count):

            @pl.when(pl.program_id(0) == k)
            def _(k=k):
                if k < 2:
                    outs[k][...] = tile
                    return
                start = 0
                for j, size in enumerate(sizes):
                    outs[2 + (k - 2) * len(sizes) + j][...] = tile[:, start : start + size]
                    start += size

    by_distance = lambda i, w: (0, w[1] ^ i)
    return pl.pallas_call(
        body,
        out_shape=[jax.ShapeDtypeStruct(shape, jnp.bfloat16) for shape in shapes]
        + [jax.ShapeDtypeStruct((1, width), jnp.float32)],
        grid_spec=pltpu.PrefetchScalarGridSpec(
            num_scalar_prefetch=1,
            grid=(dp_count,),
            in_specs=[pl.BlockSpec((tokens, own_cols), by_distance)],
            out_specs=[pl.BlockSpec(shape, lambda i, w: (0, 0)) for shape in shapes]
            + [pl.BlockSpec((1, own_cols), by_distance)],
        ),
        compiler_params=PARAMS,
        name="split_columns",
    )(where_to, gdata)


def input_gradient(gdata, down_weight):
    tokens, width = gdata.shape
    ff = down_weight.shape[0]
    tile = 256 if ff % 256 == 0 else LANES

    def body(left, right, out):
        out[...] = lax.dot_general(
            left[...], right[...], (((1,), (1,)), ((), ())), preferred_element_type=jnp.float32
        ).astype(jnp.bfloat16)

    return pl.pallas_call(
        body,
        out_shape=jax.ShapeDtypeStruct((tokens, ff), jnp.bfloat16),
        grid=(ff // tile,),
        in_specs=[pl.BlockSpec((tokens, width), lambda i: (0, 0)), pl.BlockSpec((tile, width), lambda i: (i, 0))],
        out_specs=pl.BlockSpec((tokens, tile), lambda i: (0, i)),
        cost_estimate=pl.CostEstimate(
            flops=2 * tokens * width * ff, transcendentals=0, bytes_accessed=2 * width * (tokens + ff)
        ),
        compiler_params=PARAMS,
        name="input_gradient",
    )(gdata, down_weight)


def divide(peak):
    quotient = ceiling / peak
    wide = quotient * 4097.0
    high = wide - (wide - quotient)
    rest = (ceiling - high * peak) - (quotient - high) * peak
    return quotient + rest * (quotient * (1.0 / ceiling))


def scale_tables(peaks, where_to, ff, own_cols, ctx_count):
    count = len(peaks)
    rows = ff // ctx_count
    width_cols = (peaks[0].shape[1] - ff) // ctx_count

    def body(where_ref, *refs):
        sources, rest = refs[:count], refs[count:]
        cols, gtable, hidden_amax, grad_amax, by_lane, by_row = rest
        for out, base in ((hidden_amax, 0), (grad_amax, ff)):
            size = out.shape[1]
            picked = sources[0][:, base : base + size]
            for j in range(1, ctx_count):
                other = sources[0][:, base + j * size : base + (j + 1) * size]
                picked = jnp.where(where_ref[0] == j, other, picked)
            out[...] = picked
        start = pl.multiple_of(ff + where_ref[1] * own_cols, LANES)
        for r in range(count):
            peak = sources[r][:, :ff]
            by_lane[r : r + 1, :] = divide(peak)
            by_lane[count + r : count + r + 1, :] = peak / ceiling
            peak = sources[r][:, pl.ds(start, own_cols)]
            gtable[r : r + 1, :] = divide(peak)
            gtable[count + r : count + r + 1, :] = peak / ceiling
        for c in range(0, ff, LANES):
            by_row[c : c + LANES, :] = by_lane[:, c : c + LANES].T
        for j in range(ctx_count):
            begin = pl.multiple_of((where_ref[0] ^ row_order(ctx_count)[j]) * rows, 8)
            cols[j * rows : (j + 1) * rows, :] = by_row[pl.ds(begin, rows), :]

    whole = lambda i, w: (0, 0)
    return pl.pallas_call(
        body,
        out_shape=(
            jax.ShapeDtypeStruct((ff, 2 * count), jnp.float32),
            jax.ShapeDtypeStruct((2 * count, own_cols), jnp.float32),
            jax.ShapeDtypeStruct((1, rows), jnp.float32),
            jax.ShapeDtypeStruct((1, width_cols), jnp.float32),
        ),
        grid_spec=pltpu.PrefetchScalarGridSpec(
            num_scalar_prefetch=1,
            grid=(1,),
            in_specs=[pl.BlockSpec(peaks[0].shape, whole)] * count,
            out_specs=[
                pl.BlockSpec((ff, 2 * count), whole),
                pl.BlockSpec((2 * count, own_cols), whole),
                pl.BlockSpec((1, rows), whole),
                pl.BlockSpec((1, width_cols), whole),
            ],
            scratch_shapes=[pltpu.VMEM((2 * count, ff), jnp.float32), pltpu.VMEM((ff, 2 * count), jnp.float32)],
        ),
        compiler_params=PARAMS,
        name="scale_tables",
    )(where_to, *peaks)


def quantize_rows(sources, cols, tile):
    rows, tokens = sources[0].shape
    count = len(sources)

    def body(*refs):
        cols_ref, out = refs[count:]
        for r in range(count):
            out[:, r * tokens : (r + 1) * tokens] = to_grid(
                refs[r][...], cols_ref[:, r : r + 1], cols_ref[:, count + r : count + r + 1]
            )

    by_step = lambda i: (i, 0)
    return pl.pallas_call(
        body,
        out_shape=jax.ShapeDtypeStruct((rows, count * tokens), jnp.bfloat16),
        grid=(rows // tile,),
        in_specs=[pl.BlockSpec((tile, tokens), by_step)] * count + [pl.BlockSpec((tile, 2 * count), by_step)],
        out_specs=pl.BlockSpec((tile, count * tokens), by_step),
        cost_estimate=pl.CostEstimate(
            flops=2000 * rows * tokens * count, transcendentals=0, bytes_accessed=4 * rows * tokens * count
        ),
        compiler_params=PARAMS,
        name="quantize_rows",
    )(*sources, cols)


def product(left, right):
    return lax.dot_general(left, right, (((1,), (0,)), ((), ())), preferred_element_type=jnp.float32)


def quantize_and_multiply(hq, sources, gtable, start, tile):
    rows, depth = hq.shape
    tokens, width = sources[2].shape
    count = len(sources)

    def body(*refs):
        hq_ref, table = refs[:2]
        raw = refs[2 : 2 + count]
        out, gq = refs[2 + count :]

        @pl.when(pl.program_id(0) == 0)
        def _():
            for r in range(count):
                gq[r * tokens : (r + 1) * tokens, :] = to_grid(
                    raw[r][:, start : start + width] if r < 2 else raw[r][...],
                    table[r : r + 1, start : start + width],
                    table[count + r : count + r + 1, start : start + width],
                )

        out[...] = product(hq_ref[...], gq[...]).astype(jnp.bfloat16)

    whole = lambda i: (0, 0)
    return pl.pallas_call(
        body,
        out_shape=(
            jax.ShapeDtypeStruct((rows, width), jnp.bfloat16),
            jax.ShapeDtypeStruct((depth, width), jnp.bfloat16),
        ),
        grid=(rows // tile,),
        in_specs=[pl.BlockSpec((tile, depth), lambda i: (i, 0)), pl.BlockSpec(gtable.shape, whole)]
        + [pl.BlockSpec(source.shape, whole) for source in sources],
        out_specs=[pl.BlockSpec((tile, width), lambda i: (i, 0)), pl.BlockSpec((depth, width), whole)],
        cost_estimate=pl.CostEstimate(
            flops=4 * rows * depth * width, transcendentals=0, bytes_accessed=2 * depth * (rows + width)
        ),
        compiler_params=PARAMS,
        name="quantize_and_multiply",
    )(hq, gtable, *sources)


def finish(rows_in, cols, gq, arrived, tile):
    raw = isinstance(rows_in, list)
    inputs = rows_in if raw else [rows_in]
    count = len(inputs)
    rows, tokens = inputs[0].shape
    depth, width = gq.shape
    steps = rows // tile
    cut = steps // 2

    def body(*refs):
        gq_ref, arrived_ref = refs[:2]
        sources, rest = refs[2 : 2 + count], refs[2 + count :]
        step = pl.program_id(0)
        if raw:
            cols_ref, send, keep, hq = rest
            for r in range(count):
                hq[:, r * tokens : (r + 1) * tokens] = to_grid(
                    sources[r][...], cols_ref[:, r : r + 1], cols_ref[:, count + r : count + r + 1]
                )
        else:
            send, keep = rest
            hq = sources[0]
        total = product(hq[...], gq_ref[...]) + arrived_ref[...].astype(jnp.float32)

        @pl.when(step < cut)
        def _():
            send[...] = total.astype(jnp.bfloat16)

        @pl.when(step >= cut)
        def _():
            keep[...] = total

    by_step = lambda i: (i, 0)
    in_specs = [pl.BlockSpec((depth, width), lambda i: (0, 0)), pl.BlockSpec((tile, width), by_step)]
    in_specs += [pl.BlockSpec((tile, tokens), by_step)] * count
    operands = [gq, arrived] + inputs
    out_shape = [
        jax.ShapeDtypeStruct((cut * tile, width), jnp.bfloat16),
        jax.ShapeDtypeStruct((cut * tile, width), jnp.float32),
    ]
    out_specs = [
        pl.BlockSpec((tile, width), lambda i: (jnp.minimum(i, cut - 1), 0)),
        pl.BlockSpec((tile, width), lambda i: (jnp.maximum(i - cut, 0), 0)),
    ]
    if raw:
        in_specs.append(pl.BlockSpec((tile, 2 * count), lambda i: (i + steps, 0)))
        operands.append(cols)
        out_shape.append(jax.ShapeDtypeStruct((rows, depth), jnp.bfloat16))
        out_specs.append(pl.BlockSpec((tile, depth), by_step))
    return pl.pallas_call(
        body,
        out_shape=out_shape,
        grid=(steps,),
        in_specs=in_specs,
        out_specs=out_specs,
        cost_estimate=pl.CostEstimate(
            flops=4 * rows * depth * width, transcendentals=0, bytes_accessed=2 * depth * (rows + width)
        ),
        compiler_params=PARAMS,
        name="finish",
    )(*operands)


SHARES = (0.375, 0.625, 0.875, 1.0)


def split_width(width):
    units = width // LANES
    ends = [0] + [round(units * share) for share in SHARES]
    return [(end - begin) * LANES for begin, end in zip(ends, ends[1:]) if end > begin]


def on_device(grad_out, hidden, down_weight):
    gdata = grad_out[0]
    hdata = hidden[0]
    tokens = gdata.shape[0]
    ctx_count, dp_count = lax.axis_size("ctx"), lax.axis_size("dp")
    position, place = lax.axis_index("ctx"), lax.axis_index("dp")
    ff, width = hdata.shape[1], gdata.shape[1]
    ff_rows = ff // ctx_count
    own_cols = width // dp_count
    seq_total = tokens * ctx_count * dp_count
    tile = 2 * ff_rows

    def swap(value, axis, distance):
        count = ctx_count if axis == "ctx" else dp_count
        return lax.ppermute(value, axis, [(i, i ^ distance) for i in range(count)])

    sizes = split_width(own_cols)
    starts = [sum(sizes[:j]) for j in range(len(sizes))]

    where_to = jnp.stack([position, place]).astype(jnp.int32)
    sent_rows, kept_rows, hpeak = turn_rows(hdata, where_to, ctx_count)
    own_block, near_block, *far_blocks, gpeak = split_columns(gdata, where_to, dp_count, sizes)
    near_block = swap(near_block, "dp", 1)
    chunks = []
    for j in range(len(sizes)):
        far = [swap(far_blocks[(k - 2) * len(sizes) + j], "dp", k) for k in range(2, dp_count)]
        chunks.append([own_block, near_block] + far)

    def spread(value):
        slots = [value, swap(value, "dp", 1)]
        for k in range(2, dp_count, 2):
            far = swap(value, "dp", k)
            slots += [far, swap(far, "dp", 1)]
        return slots

    sent_slots = spread(sent_rows)
    kept_slots = spread(kept_rows)

    peaks = jnp.concatenate([hpeak, gpeak], axis=1)
    bit = 1
    while bit < ctx_count:
        peaks = jnp.maximum(peaks, swap(peaks, "ctx", bit))
        bit *= 2
    peaks = jnp.maximum(peaks, 1.0)
    all_peaks = [peaks] + [swap(peaks, "dp", k) for k in range(1, dp_count)]
    cols, gtable, hidden_amax, grad_amax = scale_tables(
        all_peaks, where_to, ff, own_cols, ctx_count
    )
    hq_sent = quantize_rows(sent_slots, cols, ff_rows)
    kept_in, results = kept_slots, []
    for j, (start, size) in enumerate(zip(starts, sizes)):
        outgoing, gq = quantize_and_multiply(hq_sent, chunks[j], gtable, start, tile)
        arrived = swap(outgoing, "ctx", 1)
        send, keep, *quantized = finish(kept_in, cols, gq, arrived, ff_rows)
        kept_in = quantized[0] if quantized else kept_in
        bit = 2
        while True:
            arrived = swap(send, "ctx", bit)
            total = keep + arrived.astype(jnp.float32)
            bit *= 2
            if bit == ctx_count:
                break
            cut = total.shape[0] // 2
            send, keep = total[:cut].astype(jnp.bfloat16), total[cut:]
        results.append(total)
    weight_grad = jnp.concatenate(results, axis=1) / jnp.sqrt(jnp.float32(seq_total))

    grad_hidden = input_gradient(gdata, down_weight)[None]
    return (grad_hidden, weight_grad, hidden_amax, grad_amax)


def solution(mesh):
    placed = (P("dp", "ctx", None), P("dp", "ctx", None), P())

    return jax.shard_map(
        on_device,
        mesh=mesh,
        in_specs=placed,
        out_specs=(P("dp", "ctx", None), P("ctx", "dp"), P("dp", "ctx"), P("dp", "ctx")),
        check_vma=False,
    )
```
